32 devices in a mesh: groups: 2 (over x), expert: 8 (over z, y), seq: 2 (over core).
Axes of the slice: x: 2, y: 2, z: 4, core: 2. Of those that a mesh axis runs over, the one named last changes fastest.
Arguments:
- query: bfloat16 [16, 128, 1024], P(('groups', 'expert')), parts along dimension 0, may hold values from -160 to 160
- key_cache: bfloat16 [16, 768, 1024], P(('groups', 'expert'), 'seq'), parts along dimension 0, may hold values from -4 to 4
- value_cache: bfloat16 [16, 768, 1024], P(('groups', 'expert'), 'seq'), parts along dimension 0, may hold values from -6 to 6
- key_new: bfloat16 [16, 128, 1024], P(('groups', 'expert')), parts along dimension 0, may hold values from -6 to 6
- value_new: bfloat16 [16, 128, 1024], P(('groups', 'expert')), parts along dimension 0, may hold values from -6 to 6
- resid: bfloat16 [16, 128, 1024], P(('groups', 'expert')), parts along dimension 0, may hold values from -6 to 6
- routing: int32 [16, 128, 1], P(('groups', 'expert')), parts along dimension 0, may hold values from 0 to 7; in each aligned block of 128 rows (0 to 127, 128 to 255, ..., all dimensions but the last counted through in order) at most 48 rows name the same one
- router_prob: float32 [16, 128], P(('groups', 'expert')), parts along dimension 0, may hold values from 0.2 to 1
- out_weight: bfloat16 [1024, 1024], replicated, may hold values from -0.1875 to 0.1875
- ffn_gain: float32 [1024], replicated, may hold values from 0.5 to 2
- w_gate: bfloat16 [8, 1024, 2560], P('expert', None, 'seq'), may hold values from -0.1875 to 0.1875
- w_up: bfloat16 [8, 1024, 2560], P('expert', None, 'seq'), may hold values from -0.1875 to 0.1875
- w_down: bfloat16 [8, 2560, 1024], P('expert', 'seq'), may hold values from -0.125 to 0.125
Outputs:
- layer_out: bfloat16 [16, 128, 1024], P(('groups', 'expert')), parts along dimension 0
The draws below stay inside these ranges and needn't reach their ends.
There are 2 independent parts, one for each index of `groups`. The reference program is written for one: setup_inputs(seed, part) draws one part's arguments, and reference() takes and returns one part's arrays. A program takes and returns all parts, laid end to end along the dimension named above; an argument that names none is the same for every part. Nothing has to cross between parts.
Inputs may be any that keep to these rules, and one draw needn't show every extreme that they name: `routing`: among the 128 tokens of one sequence no expert is named more than 48 times, a bound that some block reaches.
All inputs are finite; a program needn't handle non-finite values.
Results may differ from the reference program's by a relative error of at most 0.014.
Values may be sent and summed in bfloat16 or wider, within the bound.
A program may use at most 64 MiB of HBM per device.

```python
import math
import jax
import jax.numpy as jnp
import numpy as np
from jax import lax

MODEL_WIDTH = 1024
HEADS = 16
HEAD_DIM = 64
FF = 2560
QRY = 128
CTX = 768
BATCH = 8
EXPERTS = 8
CAP = 48


def base_keys(key):
    return jnp.clip(jax.random.normal(jax.random.fold_in(key, 31), (BATCH, CTX, MODEL_WIDTH), jnp.float32), -4.0, 4.0)


def draw_key_cache(key, part):
    keys = base_keys(key)
    return keys.astype(jnp.bfloat16)


def draw_query(key, part):
    queries = 2.5 * jnp.clip(jax.random.normal(jax.random.fold_in(key, 53), (BATCH, QRY, MODEL_WIDTH), jnp.float32), -4.0, 4.0)
    return queries.astype(jnp.bfloat16)


def block_scale(stream_key, shape, pieces, least, largest):
    loudness, own = 1.0, jax.random.fold_in(stream_key, 6)
    for dim, blocks in pieces:
        heights = jnp.exp(jax.random.uniform(jax.random.fold_in(own, dim), (blocks,), jnp.float32, least / len(pieces), largest / len(pieces)))
        loudness = loudness * jnp.repeat(heights, shape[dim] // blocks).reshape([-1 if axis == dim else 1 for axis in range(len(shape))])
    return loudness


def shared_out(own_key, own, number, rows, amount, top, reach, slope):
    sequence = jax.random.permutation(own_key, amount)
    packed, usual = load_shares(amount, rows * top, reach, slope, True), load_shares(amount, rows * top, reach, slope, False)
    places = jnp.arange(amount)

    def named(lengths, rotation):
        used = int((lengths > 0).sum())
        fixed = max(1, used // 4)
        passed = fixed + (places - fixed + rotation * (used - fixed)) % max(1, amount - fixed)
        return jnp.zeros((amount,), jnp.int32).at[sequence[jnp.where(places < fixed, places, passed)]].set(jnp.asarray(lengths, jnp.int32))

    lengths = jnp.where(number % 4 == 0, named(packed, number // 4), named(usual, number - number // 4 - 1))
    mixed = jax.random.permutation(jax.random.fold_in(own, 3), amount)
    source_of, taker = mixed[0:amount // 2 * 2:2], mixed[1:amount // 2 * 2:2]
    slack = jnp.minimum(lengths[source_of] - 1, reach - lengths[taker]) // 2
    slack = jnp.where((source_of == sequence[0]) | (taker == sequence[0]) | (lengths[taker] == 0), 0, jnp.maximum(slack, 0))
    passed = jax.random.randint(jax.random.fold_in(own, 4), (amount // 2,), 0, 1 << 20) % (slack + 1)
    lengths = lengths.at[source_of].add(-passed).at[taker].add(passed)
    items = jnp.searchsorted(jnp.cumsum(lengths), jnp.arange(rows * top), side="right").astype(jnp.int32)
    grid = items.reshape(top, rows).T
    grid = grid[jax.random.permutation(jax.random.fold_in(own, 1), rows)]
    rotation = jax.random.randint(jax.random.fold_in(own, 2), (rows, 1), 0, top)
    return jnp.take_along_axis(grid, (jnp.arange(top)[None, :] + rotation) % top, axis=1)


def load_shares(number_of, total, reach, lean, full):
    loads = [(1 << 20) // math.isqrt(grade ** lean) + 1 for grade in range(1, number_of + 1)]
    largest = reach if full else min(reach, max(-(-total // number_of), total * loads[0] // sum(loads)))
    least = 1 if total - largest >= number_of - 1 else 0
    holding, surplus = [largest] + [least] * (number_of - 1), total - largest - least * (number_of - 1)
    while surplus > 0:
        candidates = [i for i in range(1, number_of) if holding[i] < largest] or [i for i in range(1, number_of) if holding[i] < reach]
        pool, left = sum([loads[i] for i in candidates]), surplus
        for i in candidates:
            extra = min(reach - holding[i], max(1, left * loads[i] // pool), surplus)
            holding[i] = holding[i] + extra
            surplus = surplus - extra
    return np.array(holding)


def noise(key, dims, scale, most, split=(), kind=jnp.bfloat16):
    drawn = jax.random.normal(key, dims, jnp.float32) * scale
    if len(split) > 0:
        drawn = block_scale(key, dims, split, -0.22, 0.18) * drawn
    return jnp.clip(drawn, min=-most, max=most).astype(kind)


def setup_inputs(seed: int = 0, part: int = 0) -> dict:
    key_of = jax.random.split(jax.random.key(seed), 14)
    own_keys = jax.random.split(jax.random.fold_in(key_of[13], part), 14)
    query = draw_query(jax.random.fold_in(jax.random.fold_in(key_of[13], part), 71), part)
    key_cache = draw_key_cache(jax.random.fold_in(jax.random.fold_in(key_of[13], part), 71), part)
    value_cache = noise(own_keys[2], (BATCH, CTX, MODEL_WIDTH), 1.0, 6.0, ((0, 8), (1, 2)))
    key_new = noise(own_keys[3], (BATCH, QRY, MODEL_WIDTH), 1.0, 6.0, ((0, 8),))
    value_new = noise(own_keys[4], (BATCH, QRY, MODEL_WIDTH), 1.0, 6.0, ((0, 8),))
    resid = noise(own_keys[5], (BATCH, QRY, MODEL_WIDTH), 1.0, 6.0, ((0, 8),))
    routing_keys = jax.random.split(jax.random.fold_in(own_keys[6], 1), BATCH * QRY // QRY)
    routing_turns = jax.random.permutation(jax.random.fold_in(own_keys[6], 3), BATCH * QRY // QRY)
    routing = jax.vmap(lambda own, number: shared_out(jax.random.fold_in(own_keys[6], 2), own, number, QRY, EXPERTS, 1, CAP, 2))(routing_keys, routing_turns).reshape((BATCH, QRY, 1))
    router_prob = jnp.clip(jnp.exp(math.log(1.0) - 1.609438 * jax.random.uniform(own_keys[7], (BATCH, QRY), jnp.float32) ** block_scale(own_keys[7], (BATCH, QRY), ((0, 8),), -0.2, 0.2)), 0.2, 1.0)
    out_weight = noise(key_of[8], (MODEL_WIDTH, MODEL_WIDTH), MODEL_WIDTH ** -0.5, 0.1875)
    ffn_gain = jnp.clip(jnp.exp(jax.random.uniform(key_of[9], (MODEL_WIDTH,), jnp.float32, math.log(0.5), math.log(2.0))), 0.5, 2.0)
    w_gate = noise(key_of[10], (EXPERTS, MODEL_WIDTH, FF), MODEL_WIDTH ** -0.5, 0.1875, ((0, 8), (2, 2)))
    w_up = noise(key_of[11], (EXPERTS, MODEL_WIDTH, FF), MODEL_WIDTH ** -0.5, 0.1875, ((0, 8), (2, 2)))
    w_down = noise(key_of[12], (EXPERTS, FF, MODEL_WIDTH), FF ** -0.5, 0.125, ((0, 8), (1, 2)))
    return dict(query=query, key_cache=key_cache, value_cache=value_cache, key_new=key_new, value_new=value_new, resid=resid, routing=routing, router_prob=router_prob, out_weight=out_weight, ffn_gain=ffn_gain, w_gate=w_gate, w_up=w_up, w_down=w_down)


def reference(query, key_cache, value_cache, key_new, value_new, resid, routing, router_prob, out_weight, ffn_gain, w_gate, w_up, w_down):
    scale = 1.0 / math.sqrt(HEAD_DIM)
    causal = jnp.arange(QRY)[None, :] <= jnp.arange(QRY)[:, None]
    allowed = jnp.concatenate([jnp.ones((QRY, CTX), dtype=bool), causal], axis=1)

    def attend(inputs):
        queries, keys_old, values_old, candidate_keys, values_fresh = inputs
        heads_q = queries.astype(jnp.float32).reshape(QRY, HEADS, HEAD_DIM)
        keys = jnp.concatenate([keys_old, candidate_keys], axis=0).astype(jnp.float32).reshape(-1, HEADS, HEAD_DIM)
        values = jnp.concatenate([values_old, values_fresh], axis=0).astype(jnp.float32).reshape(-1, HEADS, HEAD_DIM)
        scores = jnp.einsum('qhd,khd->hqk', heads_q, keys) * scale
        scores = jnp.where(allowed[None], scores, -jnp.inf)
        peak = lax.optimization_barrier(jnp.max(scores, axis=2, keepdims=True))
        expw = jnp.exp(scores - peak)
        denom = lax.optimization_barrier(jnp.sum(expw, axis=2))
        weights = lax.optimization_barrier(expw.astype(jnp.bfloat16)).astype(jnp.float32)
        weighted = jnp.einsum('hqk,khd->qhd', weights, values)
        attn = weighted / jnp.transpose(denom)[:, :, None]
        return attn.reshape(QRY, MODEL_WIDTH).astype(jnp.bfloat16)
    attn = lax.map(attend, (query, key_cache, value_cache, key_new, value_new))
    projected = jnp.dot(attn.reshape(-1, MODEL_WIDTH), out_weight, preferred_element_type=jnp.float32).reshape(BATCH, QRY, MODEL_WIDTH)
    hidden = (resid.astype(jnp.float32) + projected).astype(jnp.bfloat16)
    hidden_f = hidden.astype(jnp.float32)
    meansq = lax.optimization_barrier(jnp.mean(hidden_f * hidden_f, axis=-1, keepdims=True))
    normed = (hidden_f * lax.rsqrt(meansq + 1e-06) * ffn_gain.astype(jnp.float32)).astype(jnp.bfloat16)
    normed_features = normed.astype(jnp.float32)
    route = routing[..., 0].astype(jnp.int32)
    onehot = (route[..., None] == jnp.arange(EXPERTS, dtype=jnp.int32)).astype(jnp.int32)
    rank = lax.optimization_barrier(jnp.sum(jnp.cumsum(onehot, axis=1) * onehot, axis=-1)) - 1
    slots = jnp.arange(CAP, dtype=jnp.int32)

    def expert_step(total, item):
        index, gate_w, up_w, down_w = item
        picked = (route == index)[:, None, :] & (rank[:, None, :] == slots[None, :, None])
        expert_selection = picked.astype(jnp.float32)
        token_rows = jnp.einsum('elr,ery->ely', expert_selection, normed_features).astype(jnp.bfloat16).reshape(-1, MODEL_WIDTH)
        gate = jnp.dot(token_rows, gate_w, preferred_element_type=jnp.float32)
        upper = jnp.dot(token_rows, up_w, preferred_element_type=jnp.float32)
        act = (jax.nn.gelu(gate, approximate=True) * upper).astype(jnp.bfloat16)
        expert_result = jnp.dot(act, down_w, preferred_element_type=jnp.float32).astype(jnp.bfloat16)
        expert_result = lax.optimization_barrier(expert_result).astype(jnp.float32).reshape(BATCH, CAP, MODEL_WIDTH)
        returned_output = jnp.einsum('hio,hij->hoj', expert_selection, expert_result)
        return (total + returned_output, None)
    start = jnp.zeros((BATCH, QRY, MODEL_WIDTH), jnp.float32)
    expert_out, unused = lax.scan(expert_step, start, (jnp.arange(EXPERTS, dtype=jnp.int32), w_gate, w_up, w_down))
    return (hidden_f + router_prob.astype(jnp.float32)[..., None] * expert_out).astype(jnp.bfloat16)
```

```python
import functools
import math

import jax
import jax.numpy as jnp
from jax import lax
from jax.experimental import pallas as pl
from jax.experimental.pallas import tpu as pltpu
from jax.sharding import PartitionSpec as P

HEAD_DIM = 64
LANES = 128
MESH = pl.DeviceIdType.MESH
F32 = jnp.float32
BF16 = jnp.bfloat16


def flip(me, k):
    other, bit = me, 1
    while bit <= k:
        if k & bit:
            other = other + bit - 2 * bit * ((me // bit) % 2)
        bit *= 2
    return other


def kernel(
    cfg,
    q_hbm,
    kc_hbm,
    vc_hbm,
    kn_hbm,
    vn_hbm,
    res_hbm,
    route_ref,
    prob_ref,
    wo_hbm,
    gain_ref,
    wg_hbm,
    wu_hbm,
    wd_hbm,
    out_ref,
    q,
    kc,
    vc,
    kn,
    vn,
    res,
    wo,
    wg,
    wu,
    wd,
    o_loc,
    o_send,
    o_recv,
    o_fresh,
    st_send,
    st_recv,
    attn,
    sendb,
    xb,
    act,
    rs_send,
    rs_recv,
    ret,
    yb,
    in_sem,
    chunk_sem,
    o_sem,
    st_sem,
    disp_sem,
    fwd_sem,
    rs_sem,
    ret_sem,
    yfwd_sem,
):
    experts, capp, groups, chunks, tile = cfg
    tokens, width = q.shape
    half = width // 2
    slots = experts * capp
    hidden_units = wg.shape[1]
    heads = width // HEAD_DIM
    span = width // chunks
    me = lax.axis_index("expert")
    core = lax.axis_index("seq")
    partner = 1 - core

    def load(src, dst, sem):
        copy = pltpu.make_async_copy(src, dst, sem)
        copy.start()
        return copy

    in_chunks = []
    for j in range(chunks):
        cols = pl.ds(j * span, span)
        in_chunks.append(
            [
                load(q_hbm.at[0, :, cols], q.at[:, cols], chunk_sem.at[0, j]),
                load(kc_hbm.at[0, :, cols], kc.at[:, cols], chunk_sem.at[1, j]),
                load(vc_hbm.at[0, :, cols], vc.at[:, cols], chunk_sem.at[2, j]),
            ]
        )

    barrier = pltpu.get_barrier_semaphore()
    pl.semaphore_signal(barrier, inc=1, device_id={"seq": partner}, device_id_type=MESH)
    for k in range(1, experts):
        pl.semaphore_signal(
            barrier, inc=1, device_id={"expert": flip(me, k)}, device_id_type=MESH
        )

    loads = {}
    for i, (name, src, dst) in enumerate(
        (
            ("kn", kn_hbm.at[0], kn),
            ("vn", vn_hbm.at[0], vn),
            ("res", res_hbm.at[0], res),
            ("wo", wo_hbm, wo),
            ("wg", wg_hbm.at[0], wg),
            ("wu", wu_hbm.at[0], wu),
            ("wd", wd_hbm.at[0], wd),
        )
    ):
        loads[name] = load(src, dst, in_sem.at[i])

    route = route_ref[...]
    row_i = lax.broadcasted_iota(jnp.int32, (tokens, tokens), 0)
    col_i = lax.broadcasted_iota(jnp.int32, (tokens, tokens), 1)
    upto = (row_i <= col_i).astype(F32).astype(BF16)
    named = lax.broadcasted_iota(jnp.int32, (experts, tokens), 0) == route
    onehot = named.astype(F32)
    running = jnp.dot(onehot.astype(BF16), upto, preferred_element_type=F32)
    target = jnp.sum(running * onehot, axis=0, keepdims=True) - 1.0
    for k in range(1, experts):
        target = target + jnp.where(route == flip(me, k), float(k * capp), 0.0)
    eye = row_i == col_i
    target_col = jnp.sum(jnp.where(eye, target, 0.0), axis=1, keepdims=True)
    prob_col = jnp.sum(jnp.where(eye, prob_ref[...], 0.0), axis=1, keepdims=True)
    placer = (
        (lax.broadcasted_iota(jnp.int32, (slots, tokens), 0).astype(F32) == target)
        .astype(F32)
        .astype(BF16)
    )
    placer_t = (
        (lax.broadcasted_iota(jnp.int32, (tokens, slots), 1).astype(F32) == target_col)
        .astype(F32)
        .astype(BF16)
    )

    scale = 1.0 / math.sqrt(HEAD_DIM)
    lane = lax.broadcasted_iota(jnp.int32, (tokens, LANES), 1)
    low = lane < HEAD_DIM
    mask_a = jnp.where(low, scale, 0.0).astype(BF16)
    mask_b = jnp.where(low, 0.0, scale).astype(BF16)
    causal = col_i <= row_i
    causal = jnp.concatenate([causal.astype(F32)] * 2, axis=0) > 0.5

    def attend(p, keys, values, masked, peaks, sums):
        cols = slice(p * LANES, (p + 1) * LANES)
        both = q[:, cols]
        both = jnp.concatenate([both * mask_a, both * mask_b], axis=0)
        scores = lax.dot_general(
            both, keys[:, cols], (((1,), (1,)), ((), ())), preferred_element_type=F32
        )
        if masked:
            scores = jnp.where(causal, scores, -jnp.inf)
        peak = jnp.max(scores, axis=1, keepdims=True)
        expw = jnp.exp(scores - peak)
        total = jnp.sum(expw, axis=1, keepdims=True)
        weighted = jnp.dot(expw.astype(BF16), values[:, cols], preferred_element_type=F32)
        weighted = jnp.where(low, weighted[:tokens], weighted[tokens:])
        for i in range(2):
            rows = slice(i * tokens, (i + 1) * tokens)
            peaks = jnp.where(lane == 2 * p + i, peak[rows], peaks)
            sums = jnp.where(lane == 2 * p + i, total[rows], sums)
        return weighted, peaks, sums

    pairs = heads // 2
    per_chunk = pairs // chunks
    peak_loc = jnp.zeros((tokens, LANES), F32)
    sum_loc = jnp.ones((tokens, LANES), F32)
    o_copies = []
    for j in range(chunks):
        for copy in in_chunks[j]:
            copy.wait()
        for i in range(per_chunk):
            p = j * per_chunk + i
            weighted, peak_loc, sum_loc = attend(p, kc, vc, False, peak_loc, sum_loc)
            o_loc[:, p * LANES : (p + 1) * LANES] = weighted
            o_send[j, :, i * LANES : (i + 1) * LANES] = weighted.astype(BF16)
        if j == 0:
            pl.semaphore_wait(barrier, experts)
        copy = pltpu.make_async_remote_copy(
            src_ref=o_send.at[j],
            dst_ref=o_recv.at[j],
            send_sem=o_sem.at[0, j],
            recv_sem=o_sem.at[1, j],
            device_id={"seq": partner},
            device_id_type=MESH,
        )
        copy.start()
        o_copies.append(copy)
    st_send[...] = jnp.where(lane < HEAD_DIM, peak_loc, pltpu.roll(sum_loc, HEAD_DIM, 1))
    st_copy = pltpu.make_async_remote_copy(
        src_ref=st_send,
        dst_ref=st_recv,
        send_sem=st_sem.at[0],
        recv_sem=st_sem.at[1],
        device_id={"seq": partner},
        device_id_type=MESH,
    )
    st_copy.start()

    loads["kn"].wait()
    loads["vn"].wait()
    peak_new = jnp.zeros((tokens, LANES), F32)
    sum_new = jnp.ones((tokens, LANES), F32)
    for p in range(pairs):
        weighted, peak_new, sum_new = attend(p, kn, vn, True, peak_new, sum_new)
        o_fresh[:, p * LANES : (p + 1) * LANES] = weighted

    st_copy.wait()
    other = st_recv[...]
    peak_rem = other
    sum_rem = pltpu.roll(other, HEAD_DIM, 1)
    peak = jnp.maximum(jnp.maximum(peak_loc, peak_rem), peak_new)
    f_loc = jnp.exp(peak_loc - peak)
    f_rem = jnp.exp(peak_rem - peak)
    f_new = jnp.exp(peak_new - peak)
    inv = 1.0 / (f_loc * sum_loc + f_rem * sum_rem + f_new * sum_new)
    f_loc, f_rem, f_new = f_loc * inv, f_rem * inv, f_new * inv
    for j in range(chunks):
        o_copies[j].wait()
        for i in range(per_chunk):
            p = j * per_chunk + i
            cols = slice(p * LANES, (p + 1) * LANES)

            def spread(f):
                return jnp.where(low, f[:, 2 * p : 2 * p + 1], f[:, 2 * p + 1 : 2 * p + 2])

            value = (
                spread(f_loc) * o_loc[:, cols]
                + spread(f_rem) * o_recv[j, :, i * LANES : (i + 1) * LANES].astype(F32)
                + spread(f_new) * o_fresh[:, cols]
            )
            attn[:, cols] = value.astype(BF16)

    loads["wo"].wait()
    loads["res"].wait()
    projected = jnp.dot(attn[...], wo[...], preferred_element_type=F32)
    hidden = (res[...].astype(F32) + projected).astype(BF16)
    res[...] = hidden
    hidden_f = hidden.astype(F32)
    meansq = jnp.mean(hidden_f * hidden_f, axis=-1, keepdims=True)
    normed = (hidden_f * lax.rsqrt(meansq + 1e-06) * gain_ref[...]).astype(BF16)

    outgoing = jnp.dot(placer, normed, preferred_element_type=F32).astype(BF16)
    for h in range(2):
        block = outgoing[:, h * half : (h + 1) * half].reshape(experts, capp, half)
        sendb[h] = block
        xb[h, 0] = block[0]

    def remote(src, dst, sems, k, device):
        copy = pltpu.make_async_remote_copy(
            src_ref=src,
            dst_ref=dst,
            send_sem=sems.at[0, k],
            recv_sem=sems.at[1, k],
            device_id=device,
            device_id_type=MESH,
        )
        copy.start()
        return copy

    sent = {}
    for k in range(1, experts):
        sent[k] = remote(
            sendb.at[core, k], xb.at[core, k], disp_sem, k, {"expert": flip(me, k)}
        )
    loads["wg"].wait()
    loads["wu"].wait()
    loads["wd"].wait()

    returned = {}
    pending = []
    for g, (k0, k1) in enumerate(groups):
        rows = (k1 - k0) * capp
        forwarded = []
        for k in range(max(k0, 1), k1):
            sent[k].wait_recv()
            forwarded.append(
                remote(xb.at[core, k], xb.at[core, k], fwd_sem, k, {"seq": partner})
            )
        for copy in forwarded:
            copy.wait_recv()
        pending += forwarded

        def hidden_tile(t, carry):
            cols = pl.ds(pl.multiple_of(t * tile, tile), tile)
            left = xb[0, k0:k1].reshape(rows, half)
            right = xb[1, k0:k1].reshape(rows, half)
            x = jnp.concatenate([left, right], axis=1)
            gate = jnp.dot(x, wg[:, cols], preferred_element_type=F32)
            upper = jnp.dot(x, wu[:, cols], preferred_element_type=F32)
            act[:rows, cols] = (jax.nn.gelu(gate, approximate=True) * upper).astype(BF16)
            return carry

        lax.fori_loop(0, hidden_units // tile, hidden_tile, 0)
        theirs = pl.ds(pl.multiple_of(partner * half, half), half)
        mine = pl.ds(pl.multiple_of(core * half, half), half)
        here = pl.ds(k0 * capp, rows)
        rs_send[here, :] = jnp.dot(
            act[:rows], wd[:, theirs], preferred_element_type=F32
        ).astype(BF16)
        swap = remote(rs_send.at[here], rs_recv.at[here], rs_sem, g, {"seq": partner})
        own = jnp.dot(act[:rows], wd[:, mine], preferred_element_type=F32)
        swap.wait_recv()
        pending.append(swap)
        own = (own + rs_recv[here, :].astype(F32)).astype(BF16)
        ret[k0:k1] = own.reshape(k1 - k0, capp, half)
        for k in range(max(k0, 1), k1):
            returned[k] = remote(
                ret.at[k], yb.at[core, k], ret_sem, k, {"expert": flip(me, k)}
            )
        if k0 == 0:
            yb[core, 0] = ret[0]
            last = [remote(ret.at[0], yb.at[core, 0], yfwd_sem, 0, {"seq": partner})]

    for k in range(1, experts):
        returned[k].wait_recv()
        last.append(remote(yb.at[core, k], yb.at[core, k], yfwd_sem, k, {"seq": partner}))
    for copy in last:
        copy.wait_recv()
    y = jnp.concatenate([yb[0].reshape(slots, half), yb[1].reshape(slots, half)], axis=1)
    expert_out = jnp.dot(placer_t, y, preferred_element_type=F32)
    out_ref[...] = (res[...].astype(F32) + prob_col * expert_out).astype(BF16)
    for k in range(1, experts):
        sent[k].wait_send()
        returned[k].wait_send()
    for copy in pending + last:
        copy.wait_send()


def on_device(*args):
    (query, key_cache, value_cache, key_new, value_new, resid, routing, router_prob) = args[:8]
    (out_weight, ffn_gain, w_gate, w_up, w_down) = args[8:]
    tokens, width = query.shape[1:]
    context = key_cache.shape[1]
    hidden_units = w_gate.shape[2]
    experts = lax.axis_size("expert")
    capacity = max(2, 3 * tokens // experts)
    capp = -(-capacity // 16) * 16
    half = width // 2
    slots = experts * capp
    chunks = 4
    tile = 256 if hidden_units % 256 == 0 else 128
    groups = ((0, experts // 2), (experts // 2, experts))
    most = max(b - a for a, b in groups) * capp
    vmem = pl.BlockSpec(memory_space=pltpu.VMEM)
    hbm = pl.BlockSpec(memory_space=pl.ANY)
    dma = pltpu.SemaphoreType.DMA
    out = pl.pallas_call(
        functools.partial(kernel, (experts, capp, groups, chunks, tile)),
        out_shape=jax.ShapeDtypeStruct((tokens, width), BF16),
        in_specs=[hbm] * 6 + [vmem] * 2 + [hbm, vmem] + [hbm] * 3,
        out_specs=vmem,
        scratch_shapes=[
            pltpu.VMEM((tokens, width), BF16),
            pltpu.VMEM((context, width), BF16),
            pltpu.VMEM((context, width), BF16),
            pltpu.VMEM((tokens, width), BF16),
            pltpu.VMEM((tokens, width), BF16),
            pltpu.VMEM((tokens, width), BF16),
            pltpu.VMEM((width, width), BF16),
            pltpu.VMEM((width, hidden_units), BF16),
            pltpu.VMEM((width, hidden_units), BF16),
            pltpu.VMEM((hidden_units, width), BF16),
            pltpu.VMEM((tokens, width), F32),
            pltpu.VMEM((chunks, tokens, width // chunks), BF16),
            pltpu.VMEM((chunks, tokens, width // chunks), BF16),
            pltpu.VMEM((tokens, width), F32),
            pltpu.VMEM((tokens, LANES), F32),
            pltpu.VMEM((tokens, LANES), F32),
            pltpu.VMEM((tokens, width), BF16),
            pltpu.VMEM((2, experts, capp, half), BF16),
            pltpu.VMEM((2, experts, capp, half), BF16),
            pltpu.VMEM((most, hidden_units), BF16),
            pltpu.VMEM((slots, half), BF16),
            pltpu.VMEM((slots, half), BF16),
            pltpu.VMEM((experts, capp, half), BF16),
            pltpu.VMEM((2, experts, capp, half), BF16),
            dma((7,)),
            dma((3, chunks)),
            dma((2, chunks)),
            dma((2,)),
            dma((2, experts)),
            dma((2, experts)),
            dma((2, len(groups))),
            dma((2, experts)),
            dma((2, experts)),
        ],
        compiler_params=pltpu.CompilerParams(
            collective_id=0, has_side_effects=True, vmem_limit_bytes=60 * 1024 * 1024
        ),
    )(
        query,
        key_cache,
        value_cache,
        key_new,
        value_new,
        resid,
        routing.reshape(1, tokens),
        router_prob,
        out_weight,
        ffn_gain.reshape(1, width),
        w_gate,
        w_up,
        w_down,
    )
    return out[None]


def solution(mesh):
    in_specs = (
        P(("groups", "expert"), None, None),
        P(("groups", "expert"), "seq", None),
        P(("groups", "expert"), "seq", None),
        P(("groups", "expert"), None, None),
        P(("groups", "expert"), None, None),
        P(("groups", "expert"), None, None),
        P(("groups", "expert"), None, None),
        P(("groups", "expert"), None),
        P(),
        P(),
        P("expert", None, "seq"),
        P("expert", None, "seq"),
        P("expert", "seq", None),
    )
    out_specs = P(("groups", "expert"), None, None)
    return jax.shard_map(
        on_device, mesh=mesh, in_specs=in_specs, out_specs=out_specs, check_vma=False
    )
```

```python
import functools
import math

import jax
import jax.numpy as jnp
from jax import lax
from jax.experimental import pallas as pl
from jax.experimental.pallas import tpu as pltpu
from jax.sharding import PartitionSpec as P

HEAD_DIM = 64
LANES = 128
MESH = pl.DeviceIdType.MESH
F32 = jnp.float32
BF16 = jnp.bfloat16


def flip(me, k):
    other, bit = me, 1
    while bit <= k:
        if k & bit:
            other = other + bit - 2 * bit * ((me // bit) % 2)
        bit *= 2
    return other


def kernel(
    cfg,
    q_hbm,
    kc_hbm,
    vc_hbm,
    kn_hbm,
    vn_hbm,
    res_hbm,
    route_ref,
    prob_ref,
    wo_hbm,
    gain_ref,
    wg_hbm,
    wu_hbm,
    wd_hbm,
    out_ref,
    q,
    kc,
    vc,
    kn,
    vn,
    res,
    wo,
    wg,
    wu,
    wd,
    o_loc,
    o_send,
    o_recv,
    o_fresh,
    st_send,
    st_recv,
    attn,
    sendb,
    xb,
    act,
    rs_send,
    rs_recv,
    ret,
    yb,
    in_sem,
    first_sem,
    o_sem,
    st_sem,
    disp_sem,
    fwd_sem,
    rs_sem,
    ret_sem,
    yfwd_sem,
):
    experts, capp, groups, chunks, tile = cfg
    tokens, width = q.shape
    half = width // 2
    slots = experts * capp
    hidden_units = wg.shape[1]
    heads = width // HEAD_DIM
    me = lax.axis_index("expert")
    core = lax.axis_index("seq")
    partner = 1 - core

    def load(src, dst, sem):
        copy = pltpu.make_async_copy(src, dst, sem)
        copy.start()
        return copy

    first = [
        load(q_hbm.at[0], q, first_sem.at[0]),
        load(kc_hbm.at[0], kc, first_sem.at[1]),
        load(vc_hbm.at[0], vc, first_sem.at[2]),
    ]

    barrier = pltpu.get_barrier_semaphore()
    pl.semaphore_signal(barrier, inc=1, device_id={"seq": partner}, device_id_type=MESH)
    for k in range(1, experts):
        pl.semaphore_signal(
            barrier, inc=1, device_id={"expert": flip(me, k)}, device_id_type=MESH
        )

    loads = {}
    for i, (name, src, dst) in enumerate(
        (
            ("kn", kn_hbm.at[0], kn),
            ("vn", vn_hbm.at[0], vn),
            ("res", res_hbm.at[0], res),
            ("wo", wo_hbm, wo),
            ("wg", wg_hbm.at[0], wg),
            ("wu", wu_hbm.at[0], wu),
            ("wd", wd_hbm.at[0], wd),
        )
    ):
        loads[name] = load(src, dst, in_sem.at[i])

    route = route_ref[...]
    row_i = lax.broadcasted_iota(jnp.int32, (tokens, tokens), 0)
    col_i = lax.broadcasted_iota(jnp.int32, (tokens, tokens), 1)
    upto = (row_i <= col_i).astype(F32).astype(BF16)
    named = lax.broadcasted_iota(jnp.int32, (experts, tokens), 0) == route
    onehot = named.astype(F32)
    running = jnp.dot(onehot.astype(BF16), upto, preferred_element_type=F32)
    target = jnp.sum(running * onehot, axis=0, keepdims=True) - 1.0
    for k in range(1, experts):
        target = target + jnp.where(route == flip(me, k), float(k * capp), 0.0)
    eye = row_i == col_i
    target_col = jnp.sum(jnp.where(eye, target, 0.0), axis=1, keepdims=True)
    prob_col = jnp.sum(jnp.where(eye, prob_ref[...], 0.0), axis=1, keepdims=True)
    placer = (
        (lax.broadcasted_iota(jnp.int32, (slots, tokens), 0).astype(F32) == target)
        .astype(F32)
        .astype(BF16)
    )
    placer_t = (
        (lax.broadcasted_iota(jnp.int32, (tokens, slots), 1).astype(F32) == target_col)
        .astype(F32)
        .astype(BF16)
    )

    scale = 1.0 / math.sqrt(HEAD_DIM)
    lane = lax.broadcasted_iota(jnp.int32, (tokens, LANES), 1)
    low = lane < HEAD_DIM
    mask_a = jnp.where(low, scale, 0.0).astype(BF16)
    mask_b = jnp.where(low, 0.0, scale).astype(BF16)
    causal = col_i <= row_i
    causal = jnp.concatenate([causal.astype(F32)] * 2, axis=0) > 0.5

    def attend(p, keys, values, masked, peaks, sums):
        cols = slice(p * LANES, (p + 1) * LANES)
        both = q[:, cols]
        both = jnp.concatenate([both * mask_a, both * mask_b], axis=0)
        scores = lax.dot_general(
            both, keys[:, cols], (((1,), (1,)), ((), ())), preferred_element_type=F32
        )
        if masked:
            scores = jnp.where(causal, scores, -jnp.inf)
        peak = jnp.max(scores, axis=1, keepdims=True)
        expw = jnp.exp(scores - peak)
        total = jnp.sum(expw, axis=1, keepdims=True)
        weighted = jnp.dot(expw.astype(BF16), values[:, cols], preferred_element_type=F32)
        weighted = jnp.where(low, weighted[:tokens], weighted[tokens:])
        for i in range(2):
            rows = slice(i * tokens, (i + 1) * tokens)
            peaks = jnp.where(lane == 2 * p + i, peak[rows], peaks)
            sums = jnp.where(lane == 2 * p + i, total[rows], sums)
        return weighted, peaks, sums

    pairs = heads // 2
    per_chunk = pairs // chunks
    peak_loc = jnp.zeros((tokens, LANES), F32)
    sum_loc = jnp.ones((tokens, LANES), F32)
    o_copies = []
    for copy in first:
        copy.wait()
    for j in range(chunks):
        for i in range(per_chunk):
            p = j * per_chunk + i
            weighted, peak_loc, sum_loc = attend(p, kc, vc, False, peak_loc, sum_loc)
            o_loc[:, p * LANES : (p + 1) * LANES] = weighted
            o_send[j, :, i * LANES : (i + 1) * LANES] = weighted.astype(BF16)
        if j == 0:
            pl.semaphore_wait(barrier, experts)
        copy = pltpu.make_async_remote_copy(
            src_ref=o_send.at[j],
            dst_ref=o_recv.at[j],
            send_sem=o_sem.at[0, j],
            recv_sem=o_sem.at[1, j],
            device_id={"seq": partner},
            device_id_type=MESH,
        )
        copy.start()
        o_copies.append(copy)
    st_send[...] = jnp.where(lane < HEAD_DIM, peak_loc, pltpu.roll(sum_loc, HEAD_DIM, 1))
    st_copy = pltpu.make_async_remote_copy(
        src_ref=st_send,
        dst_ref=st_recv,
        send_sem=st_sem.at[0],
        recv_sem=st_sem.at[1],
        device_id={"seq": partner},
        device_id_type=MESH,
    )
    st_copy.start()

    loads["kn"].wait()
    loads["vn"].wait()
    peak_new = jnp.zeros((tokens, LANES), F32)
    sum_new = jnp.ones((tokens, LANES), F32)
    for p in range(pairs):
        weighted, peak_new, sum_new = attend(p, kn, vn, True, peak_new, sum_new)
        o_fresh[:, p * LANES : (p + 1) * LANES] = weighted

    st_copy.wait()
    other = st_recv[...]
    peak_rem = other
    sum_rem = pltpu.roll(other, HEAD_DIM, 1)
    peak = jnp.maximum(jnp.maximum(peak_loc, peak_rem), peak_new)
    f_loc = jnp.exp(peak_loc - peak)
    f_rem = jnp.exp(peak_rem - peak)
    f_new = jnp.exp(peak_new - peak)
    inv = 1.0 / (f_loc * sum_loc + f_rem * sum_rem + f_new * sum_new)
    f_loc, f_rem, f_new = f_loc * inv, f_rem * inv, f_new * inv
    for j in range(chunks):
        o_copies[j].wait()
        for i in range(per_chunk):
            p = j * per_chunk + i
            cols = slice(p * LANES, (p + 1) * LANES)

            def spread(f):
                return jnp.where(low, f[:, 2 * p : 2 * p + 1], f[:, 2 * p + 1 : 2 * p + 2])

            value = (
                spread(f_loc) * o_loc[:, cols]
                + spread(f_rem) * o_recv[j, :, i * LANES : (i + 1) * LANES].astype(F32)
                + spread(f_new) * o_fresh[:, cols]
            )
            attn[:, cols] = value.astype(BF16)

    loads["wo"].wait()
    loads["res"].wait()
    projected = jnp.dot(attn[...], wo[...], preferred_element_type=F32)
    hidden = (res[...].astype(F32) + projected).astype(BF16)
    res[...] = hidden
    hidden_f = hidden.astype(F32)
    meansq = jnp.mean(hidden_f * hidden_f, axis=-1, keepdims=True)
    normed = (hidden_f * lax.rsqrt(meansq + 1e-06) * gain_ref[...]).astype(BF16)

    outgoing = jnp.dot(placer, normed, preferred_element_type=F32).astype(BF16)
    for h in range(2):
        block = outgoing[:, h * half : (h + 1) * half].reshape(experts, capp, half)
        sendb[h] = block
        xb[h, 0] = block[0]

    def remote(src, dst, sems, k, device):
        copy = pltpu.make_async_remote_copy(
            src_ref=src,
            dst_ref=dst,
            send_sem=sems.at[0, k],
            recv_sem=sems.at[1, k],
            device_id=device,
            device_id_type=MESH,
        )
        copy.start()
        return copy

    sent = {}
    for k in range(1, experts):
        sent[k] = remote(
            sendb.at[core, k], xb.at[core, k], disp_sem, k, {"expert": flip(me, k)}
        )
    loads["wg"].wait()
    loads["wu"].wait()
    loads["wd"].wait()

    returned = {}
    pending = []
    for g, (k0, k1) in enumerate(groups):
        rows = (k1 - k0) * capp
        forwarded = []
        for k in range(max(k0, 1), k1):
            sent[k].wait_recv()
            forwarded.append(
                remote(xb.at[core, k], xb.at[core, k], fwd_sem, k, {"seq": partner})
            )
        for copy in forwarded:
            copy.wait_recv()
        pending += forwarded

        def hidden_tile(t):
            cols = pl.ds(t * tile, tile)
            left = xb[0, k0:k1].reshape(rows, half)
            right = xb[1, k0:k1].reshape(rows, half)
            x = jnp.concatenate([left, right], axis=1)
            gate = jnp.dot(x, wg[:, cols], preferred_element_type=F32)
            upper = jnp.dot(x, wu[:, cols], preferred_element_type=F32)
            act[:rows, cols] = (jax.nn.gelu(gate, approximate=True) * upper).astype(BF16)

        for t in range(hidden_units // tile):
            hidden_tile(t)
        theirs = pl.ds(pl.multiple_of(partner * half, half), half)
        mine = pl.ds(pl.multiple_of(core * half, half), half)
        here = pl.ds(k0 * capp, rows)
        rs_send[here, :] = jnp.dot(
            act[:rows], wd[:, theirs], preferred_element_type=F32
        ).astype(BF16)
        swap = remote(rs_send.at[here], rs_recv.at[here], rs_sem, g, {"seq": partner})
        own = jnp.dot(act[:rows], wd[:, mine], preferred_element_type=F32)
        swap.wait_recv()
        pending.append(swap)
        own = (own + rs_recv[here, :].astype(F32)).astype(BF16)
        ret[k0:k1] = own.reshape(k1 - k0, capp, half)
        for k in range(max(k0, 1), k1):
            returned[k] = remote(
                ret.at[k], yb.at[core, k], ret_sem, k, {"expert": flip(me, k)}
            )
        if k0 == 0:
            yb[core, 0] = ret[0]
            last = [remote(ret.at[0], yb.at[core, 0], yfwd_sem, 0, {"seq": partner})]

    for k in range(1, experts):
        returned[k].wait_recv()
        last.append(remote(yb.at[core, k], yb.at[core, k], yfwd_sem, k, {"seq": partner}))
    for copy in last:
        copy.wait_recv()
    y = jnp.concatenate([yb[0].reshape(slots, half), yb[1].reshape(slots, half)], axis=1)
    expert_out = jnp.dot(placer_t, y, preferred_element_type=F32)
    out_ref[...] = (res[...].astype(F32) + prob_col * expert_out).astype(BF16)
    for k in range(1, experts):
        sent[k].wait_send()
        returned[k].wait_send()
    for copy in pending + last:
        copy.wait_send()


def on_device(*args):
    (query, key_cache, value_cache, key_new, value_new, resid, routing, router_prob) = args[:8]
    (out_weight, ffn_gain, w_gate, w_up, w_down) = args[8:]
    tokens, width = query.shape[1:]
    context = key_cache.shape[1]
    hidden_units = w_gate.shape[2]
    experts = lax.axis_size("expert")
    capacity = max(2, 3 * tokens // experts)
    capp = -(-capacity // 16) * 16
    half = width // 2
    slots = experts * capp
    chunks = 2
    tile = 256 if hidden_units % 256 == 0 else 128
    groups = ((0, experts // 2), (experts // 2, 3 * experts // 4), (3 * experts // 4, experts))
    most = max(b - a for a, b in groups) * capp
    vmem = pl.BlockSpec(memory_space=pltpu.VMEM)
    hbm = pl.BlockSpec(memory_space=pl.ANY)
    dma = pltpu.SemaphoreType.DMA
    out = pl.pallas_call(
        functools.partial(kernel, (experts, capp, groups, chunks, tile)),
        out_shape=jax.ShapeDtypeStruct((tokens, width), BF16),
        in_specs=[hbm] * 6 + [vmem] * 2 + [hbm, vmem] + [hbm] * 3,
        out_specs=vmem,
        scratch_shapes=[
            pltpu.VMEM((tokens, width), BF16),
            pltpu.VMEM((context, width), BF16),
            pltpu.VMEM((context, width), BF16),
            pltpu.VMEM((tokens, width), BF16),
            pltpu.VMEM((tokens, width), BF16),
            pltpu.VMEM((tokens, width), BF16),
            pltpu.VMEM((width, width), BF16),
            pltpu.VMEM((width, hidden_units), BF16),
            pltpu.VMEM((width, hidden_units), BF16),
            pltpu.VMEM((hidden_units, width), BF16),
            pltpu.VMEM((tokens, width), F32),
            pltpu.VMEM((chunks, tokens, width // chunks), BF16),
            pltpu.VMEM((chunks, tokens, width // chunks), BF16),
            pltpu.VMEM((tokens, width), F32),
            pltpu.VMEM((tokens, LANES), F32),
            pltpu.VMEM((tokens, LANES), F32),
            pltpu.VMEM((tokens, width), BF16),
            pltpu.VMEM((2, experts, capp, half), BF16),
            pltpu.VMEM((2, experts, capp, half), BF16),
            pltpu.VMEM((most, hidden_units), BF16),
            pltpu.VMEM((slots, half), BF16),
            pltpu.VMEM((slots, half), BF16),
            pltpu.VMEM((experts, capp, half), BF16),
            pltpu.VMEM((2, experts, capp, half), BF16),
            dma((7,)),
            dma((3,)),
            dma((2, chunks)),
            dma((2,)),
            dma((2, experts)),
            dma((2, experts)),
            dma((2, len(groups))),
            dma((2, experts)),
            dma((2, experts)),
        ],
        compiler_params=pltpu.CompilerParams(
            collective_id=0, has_side_effects=True, vmem_limit_bytes=60 * 1024 * 1024
        ),
    )(
        query,
        key_cache,
        value_cache,
        key_new,
        value_new,
        resid,
        routing.reshape(1, tokens),
        router_prob,
        out_weight,
        ffn_gain.reshape(1, width),
        w_gate,
        w_up,
        w_down,
    )
    return out[None]


def solution(mesh):
    in_specs = (
        P(("groups", "expert"), None, None),
        P(("groups", "expert"), "seq", None),
        P(("groups", "expert"), "seq", None),
        P(("groups", "expert"), None, None),
        P(("groups", "expert"), None, None),
        P(("groups", "expert"), None, None),
        P(("groups", "expert"), None, None),
        P(("groups", "expert"), None),
        P(),
        P(),
        P("expert", None, "seq"),
        P("expert", None, "seq"),
        P("expert", "seq", None),
    )
    out_specs = P(("groups", "expert"), None, None)
    return jax.shard_map(
        on_device, mesh=mesh, in_specs=in_specs, out_specs=out_specs, check_vma=False
    )
```
